32 devices in a mesh: groups: 2 (over x), tensor: 16 (over z, y, core).
Axes of the slice: x: 2, y: 2, z: 4, core: 2. Of those that a mesh axis runs over, the one named last changes fastest.
Arguments:
- stem_field: float32 [8, 2, 262144], P('groups', None, 'tensor'), parts along dimension 0, may hold values from -6 to 6
- branches: float32 [4, 2, 2, 256, 256], P(None, None, None, None, 'tensor'), may hold values from -0.25 to 0.25
- branch_order: int32 [4], replicated, may hold values from 0 to 3, each once
- slice_values: int32 [8, 4], P('groups'), parts along dimension 0, may hold values from 0 to 1
Outputs:
- amplitudes: float32 [4, 262144], P('groups', 'tensor'), parts along dimension 0
The draws below stay inside these ranges and needn't reach their ends.
There are 2 independent parts, one for each index of `groups`. The reference program is written for one: setup_inputs(seed, part) draws one part's arguments, and reference() takes and returns one part's arrays. A program takes and returns all parts, laid end to end along the dimension named above; an argument that names none is the same for every part. Nothing has to cross between parts.
Inputs may be any that keep to these rules, and one draw needn't show every extreme that they name: `branch_order`: each branch is merged exactly once.
All inputs are finite; a program needn't handle non-finite values.
Results may differ from the reference program's by a relative error of at most 0.00014.
Values sent between devices are 32-bit elements; how exact they have to be, the bound alone decides.
A program may use at most 64 MiB of HBM per device.

```python
import jax
import jax.numpy as jnp
from jax import lax

S = 4
STEPS = 4
CB = 256
Q_DEV = 16384
NQ = 262144
N_TENSOR = 16


def plant(array, stream_key, low, top_value):
    shape = array.shape
    spot = [jax.random.randint(jax.random.fold_in(stream_key, axis), (), 0, shape[axis]) for axis in range(len(shape))]
    array = array.at[tuple(spot)].set(low)
    longest = shape.index(max(shape))
    spot[longest] = (spot[longest] + 1) % shape[longest]
    return array.at[tuple(spot)].set(top_value)


def steps_of(key, dims, split, smallest, largest):
    gain, own = 1.0, jax.random.fold_in(key, 6)
    for position, parts in split:
        heights = jnp.exp(jax.random.uniform(jax.random.fold_in(own, position), (parts,), jnp.float32, smallest / len(split), largest / len(split)))
        gain = gain * jnp.repeat(heights, dims[position] // parts).reshape([-1 if axis == position else 1 for axis in range(len(dims))])
    return gain


def centred(rng, dims, scale, limit, cuts=(), held_as=jnp.bfloat16):
    drawn = jax.random.normal(rng, dims, jnp.float32) * scale
    if len(cuts) > 0:
        drawn = steps_of(rng, dims, cuts, -0.22, 0.18) * drawn
    return jnp.clip(drawn, min=-limit, max=limit).astype(held_as)


def setup_inputs(seed: int = 0, part: int = 0) -> dict:
    key_of = jax.random.split(jax.random.key(seed), 5)
    part_splits = jax.random.split(jax.random.fold_in(key_of[4], part), 5)
    stem_field = centred(part_splits[0], (S, 2, NQ), 1.0, 6.0, ((2, 16),), jnp.float32)
    branches = centred(key_of[1], (STEPS, 2, 2, CB, CB), (2 * CB) ** -0.5, 0.25, ((4, 16),), jnp.float32)
    branch_order = jax.random.permutation(key_of[2], STEPS).astype(jnp.int32)
    slice_values = plant(jax.random.randint(part_splits[3], (S, STEPS), 0, 2), jax.random.fold_in(part_splits[3], 1), 0, 1).astype(jnp.int32)
    return {"stem_field": stem_field, "branches": branches, "branch_order": branch_order, "slice_values": slice_values}


def product(left, right):
    return jnp.einsum('shmi,sil->shml', left, right, precision=lax.Precision.HIGHEST)


def reference(stem_field, branches, branch_order, slice_values):
    shards = N_TENSOR
    middle = Q_DEV // CB
    current = stem_field
    for step_index in range(STEPS):
        branch_now = branches[branch_order[step_index]]
        values_now = slice_values[:, step_index]
        chosen = jnp.where((values_now == 1)[:, None, None, None], branch_now[1][None], branch_now[0][None])
        blocks = current.reshape(S, 2, shards, middle, CB)
        real_part = product(blocks[:, 0], chosen[:, 0]) - product(blocks[:, 1], chosen[:, 1])
        imag_part = product(blocks[:, 0], chosen[:, 1]) + product(blocks[:, 1], chosen[:, 0])
        combined = jnp.stack([real_part, imag_part], axis=1)
        combined = combined.reshape(S, 2, shards, middle, shards, CB // shards)
        current = combined.transpose(0, 1, 4, 2, 5, 3).reshape(S, 2, shards * Q_DEV)
    return jnp.sum(current, axis=0)
```

```python
import functools

import jax
import jax.numpy as jnp
from jax import lax
from jax.experimental import pallas as pl
from jax.experimental.pallas import tpu as pltpu
from jax.sharding import PartitionSpec as P

MESH = pl.DeviceIdType.MESH


def product(left, right):
    return jnp.einsum("smi,sil->slm", left, right, precision=lax.Precision.HIGHEST)


def combine_branch(stem_part, branch_now, values_now):
    slices, _, _, width = stem_part.shape
    chosen = jnp.where(
        (values_now == 1)[:, None, None, None], branch_now[1][None], branch_now[0][None]
    )
    real_part = product(stem_part[:, 0], chosen[:, 0]) - product(stem_part[:, 1], chosen[:, 1])
    imag_part = product(stem_part[:, 0], chosen[:, 1]) + product(stem_part[:, 1], chosen[:, 0])
    return jnp.stack([real_part, imag_part], axis=1)


def plain_device(stem_field, branches, branch_order, slice_values):
    shards = lax.axis_size("tensor")
    steps = branches.shape[0]
    width = branches.shape[3]
    current = stem_field
    for step in range(steps):
        table = lax.all_gather(
            lax.dynamic_index_in_dim(branches, branch_order[step], 0, keepdims=False),
            "tensor",
            axis=3,
            tiled=True,
        )
        slices, parts, entries = current.shape
        blocks = current.reshape(slices, parts, entries // width, width)
        combined = combine_branch(blocks, table, slice_values[:, step])
        combined = combined.reshape(slices, parts, shards, width // shards, entries // width)
        current = lax.all_to_all(
            combined, "tensor", split_axis=2, concat_axis=2, tiled=True
        ).reshape(current.shape)
    return jnp.sum(current, axis=0)


def split(value):
    high = value.astype(jnp.bfloat16)
    return high, (value - high.astype(jnp.float32)).astype(jnp.bfloat16)


def kernel(cfg, order, values, stem_hbm, branches_hbm, out, stem, table, shard, g0, g1, g2, g3, w0, w1, w2, w3, y, sent, got, fsent, fgot, turned_f,
           gather_sem, send_sem, x_sem, f_sem, xs_sem, fs_sem, in_sem):
    T, S, K, CB, M, CLO, CHI = cfg
    Z = T // 4
    gs = (g0, g1, g2, g3)
    ws = (w0, w1, w2, w3)
    gx = lax.axis_index("groups")
    me = lax.axis_index("tensor")
    core = lax.rem(me, 2)
    col = lax.rem(me // 2, 2)
    depth = me // 4
    partner = me + 1 - 2 * core
    across_y = me + 2 - 4 * col

    load_branches = pltpu.make_async_copy(branches_hbm, table, in_sem.at[0])
    load_branches.start()
    load_stem = pltpu.make_async_copy(stem_hbm, stem, in_sem.at[1])
    load_stem.start()
    barrier = pltpu.get_barrier_semaphore()
    for d in range(1, T):
        pl.semaphore_signal(barrier, inc=1, device_id=(gx, lax.rem(me + d, T)), device_id_type=MESH)
    pl.semaphore_signal(barrier, inc=1, device_id=(1 - gx, me), device_id_type=MESH)
    load_branches.wait()
    for t in range(4):
        shard[t] = table[order[t]]
    pl.semaphore_wait(barrier, T)

    started = []
    counter = [0] * 4
    ours = pl.ds(2 * gx, 2)
    theirs = pl.ds(2 - 2 * gx, 2)
    far = pl.ds(1, Z - 1)

    def push(src, dst, ssem, rsem, device):
        copy = pltpu.make_async_remote_copy(
            src_ref=src, dst_ref=dst, send_sem=ssem, recv_sem=rsem,
            device_id=device, device_id_type=MESH,
        )
        copy.start()
        started.append(copy)

    def arrived(dst, rsem):
        pltpu.make_async_remote_copy(
            src_ref=dst, dst_ref=dst, send_sem=rsem, recv_sem=rsem,
            device_id=(gx, partner), device_id_type=MESH).wait_recv()

    def token(t):
        counter[t] += 1
        return send_sem.at[t, counter[t] - 1]

    def send(t, src, dst, slot, device):
        push(src, dst, token(t), gather_sem.at[t, slot], device)

    def pair(t, row, levels, part, slot):
        send(t, gs[t].at[0, row, levels, part], gs[t].at[1, row, levels, part], slot, (gx, partner))

    def side(t, row, slot):
        src = gs[t].at[0, row, far, ours]
        send(t, src, src, slot, (1 - gx, me))

    def launch(t):
        for d in range(1, Z):
            to = lax.rem(depth + d, Z) * 4 + lax.rem(me, 4)
            send(t, shard.at[t, ours], gs[t].at[0, 0, Z - d, ours], 11 + Z - d, (gx, to))

    def lead(t):
        send(t, shard.at[t], gs[t].at[0, 1, 0], 0, (gx, across_y))
        send(t, shard.at[t], gs[t].at[1, 0, 0], 5, (gx, partner))

    def first(t):
        for d in range(1, Z):
            arrived(gs[t].at[0, 0, d, ours], gather_sem.at[t, 11 + d])
        send(t, gs[t].at[0, 0, far, ours], gs[t].at[0, 1, far, ours], 1, (gx, across_y))
        side(t, 0, 2)
        pair(t, 0, far, ours, 6)
        if t < 2:
            launch(t + 2)
            lead(t + 2)

    def second(t):
        arrived(gs[t].at[0, 1, far, ours], gather_sem.at[t, 1])
        side(t, 1, 3)
        pair(t, 1, far, ours, 7)
        arrived(gs[t].at[0, 1, 0], gather_sem.at[t, 0])
        send(t, gs[t].at[0, 1, 0], gs[t].at[1, 1, 0], 8, (gx, partner))

    def third(t):
        arrived(gs[t].at[0, 0, far, theirs], gather_sem.at[t, 2])
        pair(t, 0, far, theirs, 9)
        arrived(gs[t].at[0, 1, far, theirs], gather_sem.at[t, 3])
        pair(t, 1, far, theirs, 10)

    def settle(t):
        arrived(gs[t].at[1, 0, 0], gather_sem.at[t, 5])
        arrived(gs[t].at[1, 0, far, ours], gather_sem.at[t, 6])
        arrived(gs[t].at[1, 1, far, ours], gather_sem.at[t, 7])
        arrived(gs[t].at[1, 1, 0], gather_sem.at[t, 8])
        arrived(gs[t].at[1, 0, far, theirs], gather_sem.at[t, 9])
        arrived(gs[t].at[1, 1, far, theirs], gather_sem.at[t, 10])

    def load_tables(t):
        settle(t)
        g, w = gs[t], ws[t]
        for a in range(T):
            z, c, which = a // 4, (a // 2) % 2, a % 2
            rel = lax.rem(z - depth + Z, Z)
            row = jnp.where(col == c, 0, 1)
            other = jnp.where(core == which, 0, 1)
            for v in range(2):
                for p in range(2):
                    high, low = split(g[other, row, rel, 2 * v + p])
                    rows = slice(a * K, (a + 1) * K)
                    cols = slice(p * CB, (p + 1) * CB)
                    w[v, 0, rows, cols] = high
                    w[v, 1, rows, cols] = low
        if t >= 2 and CHI > 1:
            row = lax.broadcasted_iota(jnp.int32, (CB, CB), 0)
            lane = lax.broadcasted_iota(jnp.int32, (CB, CB), 1)
            if t == 2:
                c, lo, h = lane // (CLO * T), (lane // T) % CLO, lane % T
            else:
                lo, c, h = lane // (CHI * T), (lane // T) % CHI, lane % T
            move = (row == (lo * T + h) * CHI + c).astype(jnp.float32).astype(jnp.bfloat16)
            for v in range(2):
                for i in range(2):
                    for p in range(2):
                        cols = slice(p * CB, (p + 1) * CB)
                        w[v, i, :, cols] = jnp.dot(
                            w[v, i, :, cols], move, preferred_element_type=jnp.float32
                        ).astype(jnp.bfloat16)

    def stem_part(s, p):
        lanes = 2 * M
        pieces = CB // lanes
        return jnp.concatenate(
            [stem[s, pl.ds(2 * i + p, M, stride=2 * pieces), :] for i in range(pieces)], axis=1)

    def merge(t, v, real, imag):
        rh, rl = split(real)
        ih, il = split(imag)
        ah = jnp.concatenate([jnp.concatenate([rh, -ih], axis=1), jnp.concatenate([ih, rh], axis=1)], axis=0)
        al = jnp.concatenate([jnp.concatenate([rl, -il], axis=1), jnp.concatenate([il, rl], axis=1)], axis=0)
        dims = (((1,), (1,)), ((), ()))
        dot = functools.partial(lax.dot_general, dimension_numbers=dims,
                                preferred_element_type=jnp.float32)
        wh, wl = ws[t][v, 0], ws[t][v, 1]
        return dot(wh, ah) + (dot(wh, al) + dot(wl, ah))

    def regroup(ref, chi_major):
        rows = CB // CLO
        pieces = []
        for lo in range(CLO):
            if chi_major:
                pieces.append(jnp.concatenate(
                    [ref[pl.ds(c * CLO + lo, T, stride=K), :] for c in range(CHI)], axis=0))
            else:
                pieces.append(ref[pl.ds(lo, rows, stride=CLO), :])
        return [jnp.concatenate([b[:, p * M:(p + 1) * M] for b in pieces], axis=1) for p in range(2)]

    for t in range(2):
        launch(t)
    lead(0)
    lead(1)
    pending = [(first, 0), (first, 1), (second, 0), (second, 1), (third, 0), (first, 2), (third, 1),
               (first, 3), (second, 2), (second, 3), (third, 2), (third, 3)]

    def more(count):
        for _ in range(min(count, len(pending))):
            action, t = pending.pop(0)
            action(t)

    more(5)
    for t in range(4):
        gs[t][0, 0, 0] = shard[t]
    load_tables(0)
    load_stem.wait()
    for s in range(S):
        y[s] = merge(0, values[s, 0], stem_part(s, 0), stem_part(s, 1))
        if s % 2:
            more(1)
    load_tables(1)
    rows_of = lambda s, i: pl.ds(pl.multiple_of((s * T + i) * K, K), K)
    for s in range(S):
        real, imag = regroup(y.at[s], True)
        sent[pl.ds(s * T * K, T * K), :] = merge(1, values[s, 1], real, imag)
        for d in range(1, T):
            to = lax.rem(me + d, T)
            push(sent.at[rows_of(s, to)], got.at[rows_of(s, me)], xs_sem.at[s, d], x_sem.at[s, d], (gx, to))
        got[rows_of(s, me), :] = sent[rows_of(s, me), :]
        more(1)
    more(len(pending))
    load_tables(2)
    load_tables(3)
    sums = [None, None]
    for s in range(S):
        for d in range(1, T):
            frm = lax.rem(me - d + T, T)
            arrived(got.at[rows_of(s, frm)], x_sem.at[s, d])
        parts = [[], []]
        for hi in range(CHI):
            block = jnp.concatenate(
                [got[pl.ds(s * T * K + hi * CLO + lo, T, stride=K), :] for lo in range(CLO)], axis=0)
            turned = block.T
            for p in range(2):
                parts[p].append(jnp.concatenate(
                    [turned[(p * CHI + c) * T:(p * CHI + c + 1) * T] for c in range(CHI)], axis=1))
        real, imag = [jnp.concatenate(q, axis=0) for q in parts]
        r = merge(2, values[s, 2], real, imag)
        one = values[s, 3] == 1
        for v in range(2):
            part = jnp.where(one if v else jnp.logical_not(one), r, 0.0)
            sums[v] = part if s == 0 else sums[v] + part
    y[0] = sums[0]
    y[1] = sums[1]
    total = None
    for v in range(2):
        real, imag = regroup(y.at[v], False)
        r = merge(3, v, real, imag)
        total = r if v == 0 else total + r
    fsent[...] = total
    row_of = lambda i: pl.ds(pl.multiple_of(i * K, K), K)
    for d in range(1, T):
        to = lax.rem(me + d, T)
        push(fsent.at[row_of(to)], fgot.at[row_of(me)], fs_sem.at[d], f_sem.at[d], (gx, to))
    fgot[row_of(me), :] = fsent[row_of(me), :]
    for d in range(1, T):
        frm = lax.rem(me - d + T, T)
        arrived(fgot.at[row_of(frm)], f_sem.at[d])

    lanes = 2 * M
    width = lanes // CHI
    across = jnp.concatenate([fgot[pl.ds(c, T, stride=K), :] for c in range(K)], axis=0)
    halves = CB // lanes
    for i in range(halves):
        turned_f[i] = across[i * lanes:(i + 1) * lanes].T
    pieces = [jnp.concatenate(
        [turned_f[i, pl.ds(c, 2 * T, stride=CHI), :] for i in range(halves)], axis=1) for c in range(CHI)]
    count = CB // width
    lined = jnp.concatenate(
        [jnp.concatenate([q[:, j * width:(j + 1) * width] for q in pieces], axis=1) for j in range(count)], axis=0)
    row = lax.broadcasted_iota(jnp.int32, (lanes, lanes), 0)
    lane = lax.broadcasted_iota(jnp.int32, (lanes, lanes), 1)
    move = (row == (lane % CHI) * width + lane // CHI).astype(jnp.float32).astype(jnp.bfloat16)
    first, rest = lined.astype(jnp.bfloat16), lined
    rest = rest - first.astype(jnp.float32)
    second, third = split(rest)
    dot = functools.partial(jnp.dot, preferred_element_type=jnp.float32)
    placed = (dot(first, move) + dot(second, move)) + dot(third, move)
    for j in range(count):
        for p in range(2):
            out[pl.ds(2 * j + p, T, stride=2 * count), :] = placed[(2 * j + p) * T:(2 * j + p + 1) * T]
    for copy in started:
        copy.wait_send()


def fused_device(stem_field, branches, branch_order, slice_values):
    T = lax.axis_size("tensor")
    S, _, entries = stem_field.shape
    steps, _, _, CB, K = branches.shape
    M = entries // CB
    CLO = CB // M
    CHI = K // CLO
    lanes = 2 * M
    stem = stem_field.reshape(S, 2, entries // lanes, lanes).transpose(0, 2, 1, 3).reshape(S, 2 * entries // lanes, lanes)
    table = branches.reshape(steps, 4, CB, K).transpose(0, 1, 3, 2)
    vmem = pl.BlockSpec(memory_space=pltpu.VMEM)
    smem = pl.BlockSpec(memory_space=pltpu.SMEM)
    hbm = pl.BlockSpec(memory_space=pltpu.HBM)
    dma = pltpu.SemaphoreType.DMA
    gathers = pltpu.VMEM((2, 2, T // 4, 4, K, CB), jnp.float32)
    merged = pltpu.VMEM((2, 2, CB, 2 * CB), jnp.bfloat16)
    moved = pltpu.VMEM((T * S * K, 2 * M), jnp.float32)
    gathered = pl.pallas_call(
        functools.partial(kernel, (T, S, K, CB, M, CLO, CHI)),
        out_shape=jax.ShapeDtypeStruct((2 * entries // lanes, lanes), jnp.float32),
        in_specs=[smem, smem, hbm, hbm],
        out_specs=vmem,
        scratch_shapes=[
            pltpu.VMEM(stem.shape, jnp.float32), pltpu.VMEM(table.shape, jnp.float32), pltpu.VMEM(table.shape, jnp.float32),
            gathers, gathers, gathers, gathers,
            merged, merged, merged, merged,
            pltpu.VMEM((S, CB, 2 * M), jnp.float32),
            moved, moved,
            pltpu.VMEM((CB, 2 * M), jnp.float32),
            pltpu.VMEM((CB, 2 * M), jnp.float32),
            pltpu.VMEM((CB // (2 * M), 2 * M, 2 * M), jnp.float32),
            dma((4, 11 + T // 4)), dma((4, 11 + T // 4)),
            dma((S, T)), dma((T,)), dma((S, T)), dma((T,)), dma((2,)),
        ],
        compiler_params=pltpu.CompilerParams(collective_id=0, has_side_effects=True),
    )(branch_order, slice_values, stem, table)
    return gathered.reshape(entries // lanes, 2, lanes).transpose(1, 0, 2).reshape(2, entries)


def solution(mesh):
    def per_device(stem_field, branches, branch_order, slice_values):
        shards = lax.axis_size("tensor")
        steps, _, _, width, columns = branches.shape
        middle = stem_field.shape[2] // width
        fits = (
            mesh.shape["groups"] == 2 and shards % 8 == 0 and columns % 8 == 0 and steps == 4
            and 2 * middle == 128 and width % middle == 0 and columns % (width // middle) == 0
        )
        run = fused_device if fits else plain_device
        return run(stem_field, branches, branch_order, slice_values)

    return jax.shard_map(
        per_device,
        mesh=mesh,
        in_specs=(
            P("groups", None, "tensor"),
            P(None, None, None, None, "tensor"),
            P(),
            P("groups", None),
        ),
        out_specs=P("groups", "tensor"),
        check_vma=False,
    )
```

```python
import functools

import jax
import jax.numpy as jnp
from jax import lax
from jax.experimental import pallas as pl
from jax.experimental.pallas import tpu as pltpu
from jax.sharding import PartitionSpec as P

MESH = pl.DeviceIdType.MESH
scope = jax.named_scope


def product(left, right):
    return jnp.einsum("smi,sil->slm", left, right, precision=lax.Precision.HIGHEST)


def combine_branch(stem_part, branch_now, values_now):
    slices, _, _, width = stem_part.shape
    chosen = jnp.where(
        (values_now == 1)[:, None, None, None], branch_now[1][None], branch_now[0][None]
    )
    real_part = product(stem_part[:, 0], chosen[:, 0]) - product(stem_part[:, 1], chosen[:, 1])
    imag_part = product(stem_part[:, 0], chosen[:, 1]) + product(stem_part[:, 1], chosen[:, 0])
    return jnp.stack([real_part, imag_part], axis=1)


def plain_device(stem_field, branches, branch_order, slice_values):
    shards = lax.axis_size("tensor")
    steps = branches.shape[0]
    width = branches.shape[3]
    current = stem_field
    for step in range(steps):
        table = lax.all_gather(
            lax.dynamic_index_in_dim(branches, branch_order[step], 0, keepdims=False),
            "tensor",
            axis=3,
            tiled=True,
        )
        slices, parts, entries = current.shape
        blocks = current.reshape(slices, parts, entries // width, width)
        combined = combine_branch(blocks, table, slice_values[:, step])
        combined = combined.reshape(slices, parts, shards, width // shards, entries // width)
        current = lax.all_to_all(
            combined, "tensor", split_axis=2, concat_axis=2, tiled=True
        ).reshape(current.shape)
    return jnp.sum(current, axis=0)


def split(value):
    high = value.astype(jnp.bfloat16)
    return high, (value - high.astype(jnp.float32)).astype(jnp.bfloat16)


def flip(index, mask):
    bit = 1
    while bit <= mask:
        if mask & bit:
            index = index + bit * (1 - 2 * lax.rem(index // bit, 2))
        bit *= 2
    return index


def kernel(cfg, order, values, stem_hbm, branches_hbm, out_hbm, stem, table, out, g0, g1, g2, g3, w0, w1, w2, w3,
           y, sent, got, fsent, fgot, turned_f, gather_sem, send_sem, x_sem, f_sem, in_sem):
    T, S, K, CB, M, CLO, CHI = cfg
    Z = T // 4
    gs = (g0, g1, g2, g3)
    ws = (w0, w1, w2, w3)
    gx = lax.axis_index("groups")
    me = lax.axis_index("tensor")
    core = lax.rem(me, 2)
    depth = me // 4

    load_branches = pltpu.make_async_copy(branches_hbm, table, in_sem.at[0])
    load_branches.start()
    load_stem = pltpu.make_async_copy(stem_hbm, stem, in_sem.at[1])
    load_stem.start()
    barrier = pltpu.get_barrier_semaphore()
    for d in range(1, T):
        pl.semaphore_signal(barrier, inc=1, device_id=(gx, lax.rem(me + d, T)), device_id_type=MESH)
    pl.semaphore_signal(barrier, inc=1, device_id=(1 - gx, me), device_id_type=MESH)
    with scope("inputs"):
        load_branches.wait()
        for t in range(4):
            gs[t][me] = table[order[t]]
    with scope("barrier"):
        pl.semaphore_wait(barrier, T)

    ours = pl.ds(2 * gx, 2)
    theirs = pl.ds(2 - 2 * gx, 2)
    both = pl.ds(0, 4)
    partner = (gx, flip(me, 1))
    beside = (gx, flip(me, 2))
    across = (1 - gx, me)

    def push(src, dst, ssem, rsem, device):
        pltpu.make_async_remote_copy(
            src_ref=src, dst_ref=dst, send_sem=ssem, recv_sem=rsem,
            device_id=device, device_id_type=MESH,
        ).start()

    def arrived(dst, rsem):
        pltpu.make_async_remote_copy(
            src_ref=dst, dst_ref=dst, send_sem=rsem, recv_sem=rsem,
            device_id=partner, device_id_type=MESH).wait_recv()

    def left(src, ssem):
        pltpu.make_async_remote_copy(
            src_ref=src, dst_ref=src, send_sem=ssem, recv_sem=ssem,
            device_id=partner, device_id_type=MESH).wait_send()

    PAIR, ZT, B = 0, 1, 2
    ZO, C, XA, XC = 2, 2 + (Z - 1), 2 + 2 * (Z - 1), 2 + 3 * (Z - 1)

    def piece(t, k, row, half):
        return gs[t].at[flip(me, 4 * k + 2 * row), half]

    def send(t, ref, slot, device):
        push(ref, ref, send_sem.at[t], gather_sem.at[t, slot], device)

    def twin(t, ref):
        send(t, ref, PAIR, partner)

    def take(t, ref, slot):
        arrived(ref, gather_sem.at[t, slot])

    def launch(t):
        for k in range(1, Z):
            send(t, piece(t, 0, 0, ours), ZO + k, (gx, flip(me, 4 * k)))

    def surplus(t):
        send(t, piece(t, 0, 0, theirs), ZT, (gx, flip(me, 4)))

    def lead(t):
        send(t, piece(t, 0, 0, both), B, beside)
        twin(t, piece(t, 0, 0, both))

    def column(t, k):
        ref = piece(t, k, 0, ours)
        take(t, ref, ZO + k)
        send(t, ref, C + k, beside)
        if k > 1:
            send(t, ref, XA + k, across)
        twin(t, ref)

    def extra(t):
        ref = piece(t, 1, 0, theirs)
        take(t, ref, ZT)
        if t < 2:
            send(t, ref, XC + 1, beside)
        twin(t, ref)

    def row(t):
        ref = piece(t, 0, 1, both)
        take(t, ref, B)
        twin(t, ref)

    def corner(t, k):
        ref = piece(t, k, 1, ours)
        take(t, ref, C + k)
        if k > 1 or t >= 2:
            send(t, ref, XC + k, across)
        twin(t, ref)

    def side(t, k):
        ref = piece(t, k, 0, theirs)
        take(t, ref, XA + k)
        twin(t, ref)

    def last(t, k):
        ref = piece(t, k, 1, theirs)
        take(t, ref, XC + k)
        twin(t, ref)

    def settle(t):
        arrived(gs[t].at[pl.ds(0, T // 2)], gather_sem.at[t, PAIR])

    def load_tables(t):
        with scope(f"settle{t}"):
            settle(t)
        g, w = gs[t], ws[t]
        for a in range(T):
            for v in range(2):
                for p in range(2):
                    high, low = split(g[a, 2 * v + p])
                    rows = slice(a * K, (a + 1) * K)
                    cols = slice(p * CB, (p + 1) * CB)
                    w[v, 0, rows, cols] = high
                    w[v, 1, rows, cols] = low
        if t >= 2 and CHI > 1:
            row = lax.broadcasted_iota(jnp.int32, (CB, CB), 0)
            lane = lax.broadcasted_iota(jnp.int32, (CB, CB), 1)
            if t == 2:
                c, lo, h = lane // (CLO * T), (lane // T) % CLO, lane % T
            else:
                lo, c, h = lane // (CHI * T), (lane // T) % CHI, lane % T
            move = (row == (lo * T + h) * CHI + c).astype(jnp.float32).astype(jnp.bfloat16)
            for v in range(2):
                for i in range(2):
                    for p in range(2):
                        cols = slice(p * CB, (p + 1) * CB)
                        w[v, i, :, cols] = jnp.dot(
                            w[v, i, :, cols], move, preferred_element_type=jnp.float32
                        ).astype(jnp.bfloat16)

    def stem_part(s, p):
        lanes = 2 * M
        pieces = CB // lanes
        return jnp.concatenate(
            [stem[s, pl.ds(2 * i + p, M, stride=2 * pieces), :] for i in range(pieces)], axis=1)

    def merge(t, v, real, imag):
        rh, rl = split(real)
        ih, il = split(imag)
        ah = jnp.concatenate([jnp.concatenate([rh, -ih], axis=1), jnp.concatenate([ih, rh], axis=1)], axis=0)
        al = jnp.concatenate([jnp.concatenate([rl, -il], axis=1), jnp.concatenate([il, rl], axis=1)], axis=0)
        dims = (((1,), (1,)), ((), ()))
        dot = functools.partial(lax.dot_general, dimension_numbers=dims,
                                preferred_element_type=jnp.float32)
        wh, wl = ws[t][v, 0], ws[t][v, 1]
        return dot(wh, ah) + (dot(wh, al) + dot(wl, ah))

    def regroup(ref, chi_major):
        rows = CB // CLO
        pieces = []
        for lo in range(CLO):
            if chi_major:
                pieces.append(jnp.concatenate(
                    [ref[pl.ds(c * CLO + lo, T, stride=K), :] for c in range(CHI)], axis=0))
            else:
                pieces.append(ref[pl.ds(lo, rows, stride=CLO), :])
        return [jnp.concatenate([b[:, p * M:(p + 1) * M] for b in pieces], axis=1) for p in range(2)]

    far = range(1, Z)
    steps_of = lambda action, t, ks: [(action, t, k) for k in ks]
    cross = lambda t: steps_of(side, t, range(2, Z)) + steps_of(last, t, far)
    pending, marks = [], []

    def plan(*groups):
        for group in groups:
            pending.extend(group)
        marks.append(len(pending))

    plan(steps_of(column, 0, far), [(launch, 2), (surplus, 2), (row, 0)],
         [step for k in far for step in ((corner, 0, k), (column, 1, k))],
         [(extra, 0), (lead, 2), (launch, 3), (surplus, 3), (extra, 1), (row, 1)],
         steps_of(side, 0, range(2, Z)), steps_of(corner, 1, far), steps_of(last, 0, far))
    plan(steps_of(column, 2, far), [(lead, 3)], steps_of(side, 1, range(2, Z)), [(last, 1, 1)])
    for k in range(2, Z):
        plan([(last, 1, k)])
    fresh = len(marks)
    for k in far:
        plan([(column, 3, k)])
    plan([(extra, 2), (row, 2)], steps_of(corner, 2, far), [(extra, 3), (row, 3)], steps_of(corner, 3, far), cross(2), cross(3))
    done = [0]

    def until(count):
        while done[0] < count:
            action, *args = pending[done[0]]
            with scope(f"{action.__name__}#{'.'.join(map(str, args))}"):
                action(*args)
            done[0] += 1

    with scope("launch"):
        for t in range(2):
            launch(t)
            lead(t)
        for t in range(2):
            surplus(t)
    until(marks[0])
    with scope("lt0"):
        load_tables(0)
    load_stem.wait()
    for s in range(S):
        with scope(f"m0#{s}"):
            y[s] = merge(0, values[s, 0], stem_part(s, 0), stem_part(s, 1))
        until(marks[min(s + 1, fresh - 1)])
    until(marks[fresh - 1])
    with scope("lt1"):
        load_tables(1)
    rows_of = lambda s, i: pl.ds(pl.multiple_of((s * T + i) * K, K), K)
    for s in range(S):
        with scope(f"m1#{s}"):
            real, imag = regroup(y.at[s], True)
            sent[pl.ds(s * T * K, T * K), :] = merge(1, values[s, 1], real, imag)
        for d in range(T - 1, 0, -1):
            to = flip(me, d)
            push(sent.at[rows_of(s, to)], got.at[rows_of(s, me)], x_sem.at[S], x_sem.at[s], (gx, to))
        got[rows_of(s, me), :] = sent[rows_of(s, me), :]
        until(marks[min(fresh + s, len(marks) - 2)])
    until(len(pending))
    with scope("lt2"):
        load_tables(2)
    with scope("lt3"):
        load_tables(3)

    def third(s):
        parts = [[], []]
        for hi in range(CHI):
            block = jnp.concatenate(
                [got[pl.ds(s * T * K + hi * CLO + lo, T, stride=K), :] for lo in range(CLO)], axis=0)
            turned = block.T
            for p in range(2):
                parts[p].append(jnp.concatenate(
                    [turned[(p * CHI + c) * T:(p * CHI + c + 1) * T] for c in range(CHI)], axis=1))
        real, imag = [jnp.concatenate(q, axis=0) for q in parts]
        return merge(2, values[s, 2], real, imag)

    sums = [None, None]
    total = None
    for s in range(S):
        if s == S - 1 and s > 0:
            with scope("early"):
                for v in range(2):
                    y[v] = sums[v]
                for v in range(2):
                    r = merge(3, v, *regroup(y.at[v], False))
                    total = r if v == 0 else total + r
        with scope(f"xwait#{s}"):
            arrived(got.at[pl.ds(s * T * K, (T - 1) * K)], x_sem.at[s])
        with scope(f"m2#{s}"):
            r = third(s)
            if s < S - 1:
                one_hot = values[s, 3] == 1
                for v in range(2):
                    part = jnp.where(one_hot if v else jnp.logical_not(one_hot), r, 0.0)
                    sums[v] = part if s == 0 else sums[v] + part
            else:
                y[2] = r
    with scope("m3"):
        r = merge(3, values[S - 1, 3], *regroup(y.at[2], False))
        fsent[...] = r if total is None else total + r
    row_of = lambda i: pl.ds(pl.multiple_of(i * K, K), K)
    for d in range(T - 1, 0, -1):
        to = flip(me, d)
        push(fsent.at[row_of(to)], fgot.at[row_of(me)], f_sem.at[1], f_sem.at[0], (gx, to))
    fgot[row_of(me), :] = fsent[row_of(me), :]
    for t in range(4):
        left(gs[t].at[pl.ds(0, 4 * Z - 1)], send_sem.at[t])
    left(sent.at[pl.ds(0, S * (T - 1) * K)], x_sem.at[S])
    with scope("fwait"):
        arrived(fgot.at[pl.ds(0, (T - 1) * K)], f_sem.at[0])

    lanes = 2 * M
    width = lanes // CHI
    across = jnp.concatenate([fgot[pl.ds(c, T, stride=K), :] for c in range(K)], axis=0)
    halves = CB // lanes
    for i in range(halves):
        turned_f[i] = across[i * lanes:(i + 1) * lanes].T
    pieces = [jnp.concatenate(
        [turned_f[i, pl.ds(c, 2 * T, stride=CHI), :] for i in range(halves)], axis=1) for c in range(CHI)]
    count = CB // width
    lined = jnp.concatenate(
        [jnp.concatenate([q[:, j * width:(j + 1) * width] for q in pieces], axis=1) for j in range(count)], axis=0)
    row = lax.broadcasted_iota(jnp.int32, (lanes, lanes), 0)
    lane = lax.broadcasted_iota(jnp.int32, (lanes, lanes), 1)
    move = (row == (lane % CHI) * width + lane // CHI).astype(jnp.float32).astype(jnp.bfloat16)
    first, rest = lined.astype(jnp.bfloat16), lined
    rest = rest - first.astype(jnp.float32)
    second, third = split(rest)
    dot = functools.partial(jnp.dot, preferred_element_type=jnp.float32)
    placed = (dot(first, move) + dot(second, move)) + dot(third, move)
    for j in range(count):
        for p in range(2):
            out[pl.ds(2 * j + p, T, stride=2 * count), :] = placed[(2 * j + p) * T:(2 * j + p + 1) * T]
    store = pltpu.make_async_copy(out, out_hbm, in_sem.at[2])
    store.start()
    left(fsent.at[pl.ds(0, (T - 1) * K)], f_sem.at[1])
    with scope("store"):
        store.wait()


def fused_device(stem_field, branches, branch_order, slice_values):
    T = lax.axis_size("tensor")
    S, _, entries = stem_field.shape
    steps, _, _, CB, K = branches.shape
    M = entries // CB
    CLO = CB // M
    CHI = K // CLO
    lanes = 2 * M
    stem = stem_field.reshape(S, 2, entries // lanes, lanes).transpose(0, 2, 1, 3).reshape(S, 2 * entries // lanes, lanes)
    table = branches.reshape(steps, 4, CB, K).transpose(0, 1, 3, 2)
    smem = pl.BlockSpec(memory_space=pltpu.SMEM)
    hbm = pl.BlockSpec(memory_space=pltpu.HBM)
    dma = pltpu.SemaphoreType.DMA
    gathers = pltpu.VMEM((T, 4, K, CB), jnp.float32)
    merged = pltpu.VMEM((2, 2, CB, 2 * CB), jnp.bfloat16)
    moved = pltpu.VMEM((T * S * K, 2 * M), jnp.float32)
    gathered = pl.pallas_call(
        functools.partial(kernel, (T, S, K, CB, M, CLO, CHI)),
        out_shape=jax.ShapeDtypeStruct((2 * entries // lanes, lanes), jnp.float32),
        in_specs=[smem, smem, hbm, hbm],
        out_specs=hbm,
        scratch_shapes=[
            pltpu.VMEM(stem.shape, jnp.float32), pltpu.VMEM(table.shape, jnp.float32),
            pltpu.VMEM((2 * entries // lanes, lanes), jnp.float32),
            gathers, gathers, gathers, gathers,
            merged, merged, merged, merged,
            pltpu.VMEM((S, CB, 2 * M), jnp.float32),
            moved, moved,
            pltpu.VMEM((CB, 2 * M), jnp.float32),
            pltpu.VMEM((CB, 2 * M), jnp.float32),
            pltpu.VMEM((CB // (2 * M), 2 * M, 2 * M), jnp.float32),
            dma((4, 2 + 4 * (T // 4))), dma((4,)), dma((S + 1,)), dma((2,)), dma((3,)),
        ],
        compiler_params=pltpu.CompilerParams(collective_id=0, has_side_effects=True),
    )(branch_order, slice_values, stem, table)
    return gathered.reshape(entries // lanes, 2, lanes).transpose(1, 0, 2).reshape(2, entries)


def solution(mesh):
    def per_device(stem_field, branches, branch_order, slice_values):
        shards = lax.axis_size("tensor")
        steps, _, _, width, columns = branches.shape
        middle = stem_field.shape[2] // width
        fits = (
            mesh.shape["groups"] == 2 and shards % 8 == 0 and shards & (shards - 1) == 0 and columns % 8 == 0 and steps == 4
            and 2 * middle == 128 and width % middle == 0 and columns % (width // middle) == 0
        )
        run = fused_device if fits else plain_device
        return run(stem_field, branches, branch_order, slice_values)

    return jax.shard_map(
        per_device,
        mesh=mesh,
        in_specs=(
            P("groups", None, "tensor"),
            P(None, None, None, None, "tensor"),
            P(),
            P("groups", None),
        ),
        out_specs=P("groups", "tensor"),
        check_vma=False,
    )
```
